8 devices in a mesh: dp: 1 (over z), ep: 2 (over y), tp: 4 (over x, core).
Axes of the slice: x: 2, y: 2, z: 1, core: 2. Of those that a mesh axis runs over, the one named last changes fastest.
Arguments:
- tokens: bfloat16 [1024, 896], P(('dp', 'ep', 'tp'))
- expert_ids: int32 [1024, 8], P(('dp', 'ep', 'tp'))
- gates: float32 [1024, 8], P(('dp', 'ep', 'tp'))
- w_gate: bfloat16 [64, 896, 2560], P('ep', None, 'tp')
- w_up: bfloat16 [64, 896, 2560], P('ep', None, 'tp')
- w_down: bfloat16 [64, 2560, 896], P('ep', 'tp')
Outputs:
- output: bfloat16 [1024, 896], P(('dp', 'ep', 'tp'))
All inputs are finite; a program needn't handle non-finite values.
Results may differ from the reference program's by a relative error of at most 0.0102111.
Values are sent between devices in bfloat16 or wider.
A program may use at most 1 GiB of HBM per device.

```python
import jax
import jax.numpy as jnp
from jax import lax

D_MODEL = 896
FF_DIM = 2560
EXPERTS = 64
TOP_K = 8
TOK_DEV = 128
SOURCES = 8

CAPACITY = 5 * TOP_K * TOK_DEV // (4 * EXPERTS)
TOK_PART = SOURCES * TOK_DEV


def draw_routes(dev_key):
    key_perm, key_rot, key_lab = jax.random.split(dev_key, 3)
    fair_share = TOP_K * TOK_DEV // EXPERTS
    row_order = jax.random.permutation(key_perm, TOK_DEV)
    rotate = jax.random.randint(key_rot, (TOK_DEV, 1), 0, TOP_K)
    col_pos = (jnp.arange(TOP_K)[None, :] + rotate) % TOP_K
    labels = (row_order[:, None] * TOP_K + col_pos) % EXPERTS
    free_rows = jnp.logical_not(jnp.any(labels == 0, axis=1)).astype(jnp.int32)
    chosen = jnp.logical_and(free_rows > 0, jnp.cumsum(free_rows) <= fair_share // 2)
    first_col = (jnp.arange(TOP_K) == 0)[None, :]
    labels = jnp.where(jnp.logical_and(chosen[:, None], first_col), 0, labels)
    relabel = jax.random.permutation(key_lab, EXPERTS)
    return relabel[labels].astype(jnp.int32)


def setup_inputs(seed: int = 0, part: int = 0) -> dict:
    part_key = jax.random.fold_in(jax.random.key(seed), part)
    key_x, key_idx, key_gate = jax.random.split(part_key, 3)
    key_w1, key_w3, key_w2 = jax.random.split(jax.random.key(seed + 1), 3)
    tokens = jax.random.normal(key_x, (TOK_PART, D_MODEL), jnp.float32).astype(jnp.bfloat16)
    expert_ids = jax.vmap(draw_routes)(jax.random.split(key_idx, SOURCES)).reshape(TOK_PART, TOP_K)
    gates = jax.random.uniform(key_gate, (TOK_PART, TOP_K), jnp.float32, 0.5, 1.5) * TOP_K ** -0.5
    w_gate = (jax.random.normal(key_w1, (EXPERTS, D_MODEL, FF_DIM), jnp.float32) * D_MODEL ** -0.5).astype(jnp.bfloat16)
    w_up = (jax.random.normal(key_w3, (EXPERTS, D_MODEL, FF_DIM), jnp.float32) * D_MODEL ** -0.5).astype(jnp.bfloat16)
    w_down = (jax.random.normal(key_w2, (EXPERTS, FF_DIM, D_MODEL), jnp.float32) * FF_DIM ** -0.5).astype(jnp.bfloat16)
    return {"tokens": tokens, "expert_ids": expert_ids, "gates": gates, "w_gate": w_gate, "w_up": w_up, "w_down": w_down}


def slot_numbers(routes):
    hit_count = jnp.sum((routes[:, :, None] == jnp.arange(EXPERTS)).astype(jnp.int32), axis=1)
    before = jnp.cumsum(hit_count, axis=0) - hit_count
    return jnp.take_along_axis(before, routes, axis=1)


def dispatch_rows(dev_rows, dest_slot):
    row_ids = jnp.broadcast_to(jnp.arange(TOK_DEV, dtype=jnp.int32)[:, None], dest_slot.shape)
    owner_row = jnp.full((EXPERTS * CAPACITY,), TOK_DEV, jnp.int32).at[dest_slot.reshape(-1)].set(row_ids.reshape(-1), mode="drop")
    return jnp.take(dev_rows, owner_row, axis=0, mode="fill", fill_value=0).reshape(EXPERTS, CAPACITY, D_MODEL)


def expert_ffn(blk_rows, gate_mat, up_mat, down_mat):
    act_gate = jnp.dot(blk_rows, gate_mat, preferred_element_type=jnp.float32)
    act_up = jnp.dot(blk_rows, up_mat, preferred_element_type=jnp.float32)
    hidden = (jax.nn.silu(act_gate) * act_up).astype(jnp.bfloat16)
    return jnp.dot(hidden, down_mat, preferred_element_type=jnp.float32).astype(jnp.bfloat16)


def reference(tokens, expert_ids, gates, w_gate, w_up, w_down):
    dev_rows = tokens.reshape(SOURCES, TOK_DEV, D_MODEL)
    routes = expert_ids.reshape(SOURCES, TOK_DEV, TOP_K)
    dev_gates = gates.reshape(SOURCES, TOK_DEV, TOP_K)
    slot_ids = jax.vmap(slot_numbers)(routes)
    kept_mask = slot_ids < CAPACITY
    dest_slot = jnp.where(kept_mask, routes * CAPACITY + slot_ids, EXPERTS * CAPACITY)
    buffers = jax.vmap(dispatch_rows)(dev_rows, dest_slot)

    def per_expert(operands):
        blocks, gate_mat, up_mat, down_mat = operands
        return lax.map(lambda one_block: expert_ffn(one_block, gate_mat, up_mat, down_mat), blocks)

    results = lax.map(per_expert, (jnp.swapaxes(buffers, 0, 1), w_gate, w_up, w_down))
    out_table = jnp.swapaxes(results, 0, 1).reshape(SOURCES, EXPERTS * CAPACITY, D_MODEL)
    picked = jax.vmap(lambda src_table, src_dest: jnp.take(src_table, src_dest, axis=0, mode="fill", fill_value=0))(out_table, dest_slot)
    gate_kept = jnp.where(kept_mask, dev_gates, 0.0)
    mixed_rows = jnp.sum(gate_kept[..., None] * picked.astype(jnp.float32), axis=2)
    return mixed_rows.astype(jnp.bfloat16).reshape(TOK_PART, D_MODEL)
```

```python
import functools

import jax
import jax.numpy as jnp
from jax import lax
from jax.experimental import pallas as pl
from jax.experimental.pallas import tpu as pltpu
from jax.sharding import PartitionSpec as P

MESH = pl.DeviceIdType.MESH
BF16 = jnp.bfloat16
F32 = jnp.float32

SOURCES = 8
MAIN = 16
BLOCK = 4
RING = 12
WIDE = 256
NO_SLOT = 255.0

TO_PARTNER, X_LOW, X_HIGH, Y_HIGH, Y_LOW, DIAG_Y, DIAG_X, PASS_X, PASS_Y, PASS_D = range(10)
META_P, META_X, META_Y, META_D, META_PX, META_PY, META_PD = range(10, 17)
FIRST_SUM = 17
OWN, XN, DIAG, YN = range(4)
PLACE = (OWN, XN, YN, DIAG)


def iota(shape, dim):
    return lax.broadcasted_iota(jnp.int32, shape, dim)


def kernel(
    ids_ref, gates_ref, tok_hbm, wg_hbm, wu_hbm, wd_hbm, out_ref,
    xg, mg, val, spread, gmat, xe, hid, ring, away, home, got, rx1, ry1, rx2, ry2, via_x, via_y,
    own_sem, wsem, ssem, rsem,
):
    top_k, tok = ids_ref.shape
    experts = wg_hbm.shape[0]
    d_model, ff = wg_hbm.shape[1:]
    half = tok // 2
    rest = 4
    ep, tp = lax.axis_index("ep"), lax.axis_index("tp")
    partner = {"tp": tp + 1 - 2 * (tp % 2)}
    xn = {"tp": (tp + 2) % 4}
    yn = {"ep": 1 - ep}
    first_expert = ep * experts

    chunks = []
    start = 0
    while start < d_model:
        chunks.append((start, min(WIDE, d_model - start)))
        start += WIDE
    n_chunks = len(chunks)

    per_slot = 4
    groups = experts // per_slot

    def load_up(e, slot):
        return [
            pltpu.make_async_copy(wg_hbm.at[e], ring.at[slot, 0], wsem.at[slot, 0]),
            pltpu.make_async_copy(wu_hbm.at[e], ring.at[slot, 1], wsem.at[slot, 1]),
        ]

    def down_view(slot, k, width):
        per_plane = 2 if width == WIDE else 4
        return ring.at[slot, k // per_plane, pl.ds(0, ff), pl.ds((k % per_plane) * width, width)]

    def load_down(first, column, width, slot):
        count = per_slot if width == WIDE else 2 * per_slot
        return [
            pltpu.make_async_copy(
                wd_hbm.at[first + k, :, pl.ds(column, width)], down_view(slot, k, width), wsem.at[slot, k]
            )
            for k in range(count)
        ]

    n_up = experts // BLOCK
    per_chunk = groups // BLOCK

    def down_block(b):
        lb = b - n_up
        c = lb // per_chunk if lb < per_chunk * (n_chunks - 1) else n_chunks - 1
        return c, (lb - c * per_chunk) * BLOCK * per_slot

    def start_down(b):
        c, first = down_block(b)
        column, width = chunks[c]
        step = per_slot if width == WIDE else 2 * per_slot
        for i in range(BLOCK):
            for copy in load_down(first + i * step, column, width, (b * BLOCK + i) % RING):
                copy.start()

    for s in range(RING):
        for copy in load_up(s, s):
            copy.start()
    own = pltpu.make_async_copy(tok_hbm, xg.at[0], own_sem)
    own.start()

    mg[0, 0:top_k, :] = ids_ref[...].astype(F32)
    mg[0, top_k:, :] = gates_ref[...]

    def message(i, src, dst, dev):
        return pltpu.make_async_remote_copy(
            src_ref=src, dst_ref=dst, send_sem=ssem.at[i], recv_sem=rsem.at[i], device_id=dev, device_id_type=MESH
        )

    low, high = pl.ds(0, half), pl.ds(half, half)
    sent = {
        TO_PARTNER: message(TO_PARTNER, xg.at[0], xg.at[1], partner),
        X_LOW: message(X_LOW, xg.at[0, low], xg.at[2, low], xn),
        X_HIGH: message(X_HIGH, xg.at[0, high], xg.at[2, high], xn),
        Y_HIGH: message(Y_HIGH, xg.at[0, high], xg.at[4, high], yn),
        Y_LOW: message(Y_LOW, xg.at[0, low], xg.at[4, low], yn),
        DIAG_Y: message(DIAG_Y, xg.at[2, low], xg.at[6, low], yn),
        DIAG_X: message(DIAG_X, xg.at[4, high], xg.at[6, high], xn),
        PASS_X: message(PASS_X, xg.at[2], xg.at[3], partner),
        PASS_Y: message(PASS_Y, xg.at[4], xg.at[5], partner),
        PASS_D: message(PASS_D, xg.at[6], xg.at[7], partner),
        META_P: message(META_P, mg.at[0], mg.at[1], partner),
        META_X: message(META_X, mg.at[0], mg.at[2], xn),
        META_Y: message(META_Y, mg.at[0], mg.at[4], yn),
        META_D: message(META_D, mg.at[2], mg.at[6], yn),
        META_PX: message(META_PX, mg.at[2], mg.at[3], partner),
        META_PY: message(META_PY, mg.at[4], mg.at[5], partner),
        META_PD: message(META_PD, mg.at[6], mg.at[7], partner),
    }

    barrier = pltpu.get_barrier_semaphore()
    for dev in (partner, xn, yn):
        pl.semaphore_signal(barrier, inc=1, device_id=dev, device_id_type=MESH)
    row, col = iota(spread.shape, 0), iota(spread.shape, 1)
    spread[...] = jnp.where(row == col // MAIN, 1.0, 0.0).astype(BF16)
    pl.semaphore_wait(barrier, 3)
    for i in (META_P, META_X, META_Y):
        sent[i].start()
    own.wait()
    for i in (X_LOW, Y_HIGH, X_HIGH, Y_LOW, TO_PARTNER):
        sent[i].start()

    earlier = jnp.where(iota((tok, tok), 0) < iota((tok, tok), 1), 1.0, 0.0).astype(BF16)
    expert_row = (iota((experts, tok), 0) + first_expert).astype(F32)
    n_main = experts * MAIN
    lane = iota((tok, n_main), 1)

    def route(r):
        hit = jnp.zeros((experts, tok), F32)
        gate = jnp.zeros((experts, tok), F32)
        for j in range(top_k):
            here = mg[r, j : j + 1, :] == expert_row
            hit = jnp.where(here, 1.0, hit)
            gate = jnp.where(here, mg[r, top_k + j : top_k + j + 1, :], gate)
        before = jnp.dot(hit.astype(BF16), earlier, preferred_element_type=F32)
        slot = jnp.where(hit > 0.5, before, NO_SLOT)
        val[r] = slot
        g_hi = gate.astype(BF16).astype(F32)
        g_mid = (gate - g_hi).astype(BF16).astype(F32)
        g_lo = gate - g_hi - g_mid
        stack = jnp.concatenate([slot, g_hi, g_mid, g_lo], axis=0)
        by_token = stack.T.astype(BF16)
        wide = jnp.dot(by_token, spread[...], preferred_element_type=F32)
        slot_of = wide[:, 0:n_main]
        in_main = slot_of == (lane % MAIN).astype(F32)
        mine = (lane % MAIN) // rest == r % 4
        in_rest = slot_of == jnp.where(mine, MAIN + lane % rest, -1).astype(F32)
        for k in range(3):
            piece = wide[:, (k + 1) * n_main : (k + 2) * n_main]
            rows = pl.ds(k * tok, tok)
            gmat[r, rows, 0:n_main] = jnp.where(in_main, piece, 0.0).astype(BF16)
            gmat[r, rows, n_main:] = jnp.where(in_rest, piece, 0.0).astype(BF16)

    def one_hot(slots, want, e):
        line = jnp.broadcast_to(slots[e : e + 1, :], want.shape)
        return jnp.where(line == want, 1.0, 0.0).astype(BF16)

    def dispatch(sources, want, rows, batch):
        slots = jnp.concatenate([val[r] for r in sources], axis=1)
        x = xg[sources[0] : sources[-1] + 1].reshape(len(sources) * tok, d_model)
        height = want.shape[0]
        for e in range(0, experts, batch):
            pick = jnp.concatenate([one_hot(slots, want, e + i) for i in range(batch)], axis=0)
            placed = jnp.dot(pick, x, preferred_element_type=F32).astype(BF16)
            xe[e : e + batch, rows : rows + height, :] = placed.reshape(batch, height, d_model)

    def dispatch_pair(p):
        shape = (2 * MAIN, 2 * tok)
        i, l = iota(shape, 0), iota(shape, 1)
        want = jnp.where(i // MAIN == l // tok, i % MAIN, -1).astype(F32)
        dispatch([2 * p, 2 * p + 1], want, 2 * MAIN * p, 8)

    def dispatch_rest(q):
        shape = (4 * rest, 4 * tok)
        i, l = iota(shape, 0), iota(shape, 1)
        want = jnp.where(i // rest == l // tok, MAIN + i % rest, -1).astype(F32)
        dispatch([4 * q + i for i in range(4)], want, MAIN * SOURCES + 4 * rest * q, 16)

    def route_range(lo, hi):
        @pl.loop(lo, hi)
        def _(r):
            route(r)

    sent[META_P].wait_recv()
    route_range(0, 2)
    sent[TO_PARTNER].wait_recv()
    dispatch_pair(0)
    sent[META_X].wait_recv()
    sent[META_D].start()
    sent[META_PX].start()
    sent[META_Y].wait_recv()
    sent[META_PY].start()
    sent[X_LOW].wait_recv()
    sent[DIAG_Y].start()
    sent[Y_HIGH].wait_recv()
    sent[DIAG_X].start()
    sent[META_D].wait_recv()
    sent[META_PD].start()
    sent[META_PX].wait_recv()
    sent[META_PY].wait_recv()
    route_range(2, 6)
    sent[X_HIGH].wait_recv()
    sent[PASS_X].start()
    sent[Y_LOW].wait_recv()
    sent[PASS_Y].start()
    sent[META_PD].wait_recv()
    route_range(6, 8)
    sent[PASS_X].wait_recv()
    dispatch_pair(1)
    sent[PASS_Y].wait_recv()
    dispatch_pair(2)
    sent[DIAG_Y].wait_recv()
    sent[DIAG_X].wait_recv()
    sent[PASS_D].start()
    dispatch_rest(0)
    sent[PASS_D].wait_recv()
    dispatch_pair(3)
    dispatch_rest(1)

    full = ff // WIDE * WIDE

    def up_block(b):
        base = (b * BLOCK) % RING
        for i in range(BLOCK):
            for copy in load_up(b * BLOCK + i, base + i):
                copy.wait()
        for i in range(BLOCK):
            e, slot = b * BLOCK + i, base + i
            x = xe[e]
            a = jnp.dot(x, ring[slot, 0, :, 0:full], preferred_element_type=F32)
            u = jnp.dot(x, ring[slot, 1, :, 0:full], preferred_element_type=F32)
            hid[e, :, 0:full] = (jax.nn.silu(a) * u).astype(BF16)
            tail = jnp.concatenate([ring[slot, 0, :, full:], ring[slot, 1, :, full:]], axis=1)
            t = jnp.dot(x, tail, preferred_element_type=F32)
            hid[e, :, full:] = (jax.nn.silu(t[:, : ff - full]) * t[:, ff - full :]).astype(BF16)

    ahead = RING // BLOCK

    @pl.loop(0, n_up - ahead)
    def _(b):
        up_block(b)
        for i in range(BLOCK):
            for copy in load_up((b + ahead) * BLOCK + i, (b * BLOCK) % RING + i):
                copy.start()

    for b in range(n_up - ahead, n_up):
        up_block(b)
        start_down(b + ahead)

    n_blocks = n_up + per_chunk * (n_chunks - 1) + 1

    def down(b, lo, hi):
        c, first = down_block(b)
        column, width = chunks[c]
        step = per_slot if width == WIDE else 2 * per_slot
        put = (c % 2) * WIDE
        for i in range(lo, hi):
            for copy in load_down(first + i * step, column, width, (b * BLOCK + i) % RING):
                copy.wait()
        for i in range(lo, hi):
            for k in range(step):
                e = first + i * step + k
                w = down_view((b * BLOCK + i) % RING, k, width)[...]
                y = jnp.dot(hid[e], w, preferred_element_type=F32)
                xe[e, :, put : put + width] = y.astype(BF16)
        if hi == BLOCK and b + ahead < n_blocks:
            start_down(b + ahead)

    def gated(r, c):
        width = chunks[c][1]
        put = (c % 2) * WIDE
        top = MAIN * r
        bottom = MAIN * SOURCES + 4 * rest * (r // 4)
        y = jnp.concatenate(
            [
                xe[:, top : top + MAIN, put : put + width].reshape(n_main, width),
                xe[:, bottom : bottom + 4 * rest, put : put + width].reshape(n_main, width),
            ],
            axis=0,
        )
        s = jnp.dot(gmat[r], y, preferred_element_type=F32)
        return s[0:tok] + s[tok : 2 * tok] + s[2 * tok :]

    def cols(c):
        return pl.ds(*chunks[c])

    def sums(kind, c):
        i = FIRST_SUM + 5 * c + kind
        if kind == 0:
            return message(i, away.at[:, :, cols(c)], got.at[:, :, cols(c)], partner)
        if kind == 1:
            return message(i, home.at[pl.ds(XN, 2), low, cols(c)], rx1.at[:, :, cols(c)], xn)
        if kind == 2:
            return message(i, home.at[pl.ds(DIAG, 2), high, cols(c)], ry1.at[:, :, cols(c)], yn)
        if kind == 3:
            return message(i, via_y.at[:, cols(c)], ry2.at[:, cols(c)], yn)
        return message(i, via_x.at[:, cols(c)], rx2.at[:, cols(c)], xn)

    def combine_away(c):
        for r in range(1, SOURCES, 2):
            away[PLACE[r // 2], :, cols(c)] = gated(r, c)

    def combine_home(c):
        sums(0, c).start()
        for r in range(0, SOURCES, 2):
            home[PLACE[r // 2], :, cols(c)] = gated(r, c)

    def chip_sum(c):
        sums(0, c).wait_recv()
        for d in range(4):
            home[d, :, cols(c)] += got[d, :, cols(c)]
        sums(1, c).start()
        sums(2, c).start()

    def pass_on(c):
        sums(1, c).wait_recv()
        via_y[:, cols(c)] = home[YN, low, cols(c)] + rx1[1, :, cols(c)]
        sums(3, c).start()
        sums(2, c).wait_recv()
        via_x[:, cols(c)] = home[XN, high, cols(c)] + ry1[0, :, cols(c)]
        sums(4, c).start()

    def finish(c):
        sums(3, c).wait_recv()
        out_ref[low, cols(c)] = (home[OWN, low, cols(c)] + rx1[0, :, cols(c)] + ry2[:, cols(c)]).astype(BF16)
        sums(4, c).wait_recv()
        out_ref[high, cols(c)] = (home[OWN, high, cols(c)] + ry1[1, :, cols(c)] + rx2[:, cols(c)]).astype(BF16)

    b = n_up
    for c in range(n_chunks):
        if c < n_chunks - 1:
            parts = [(b + i, 0, BLOCK) for i in range(per_chunk)]
            b += per_chunk
        else:
            parts = [(b, 0, BLOCK // 2), (b, BLOCK // 2, BLOCK)]
        for n, part in enumerate(parts):
            down(*part)
            if n == 0 and c >= 1:
                chip_sum(c - 1)
            if n == 1 and c >= 2:
                pass_on(c - 2)
        combine_away(c)
        combine_home(c)
    last = n_chunks - 1
    chip_sum(last)
    pass_on(last - 1)
    for c in range(last - 1):
        finish(c)
    pass_on(last)
    finish(last - 1)
    finish(last)

    for i in range(FIRST_SUM):
        sent[i].wait_send()
    for c in range(n_chunks):
        for kind in range(5):
            sums(kind, c).wait_send()


def solution(mesh):
    ep_size, tp_size = mesh.shape["ep"], mesh.shape["tp"]
    row_spec = P(("dp", "ep", "tp"), None)

    def local_layer(tokens, expert_ids, gates, w_gate, w_up, w_down):
        tok, d_model = tokens.shape
        top_k = expert_ids.shape[1]
        experts, _, ff = w_gate.shape
        capacity = 5 * top_k * tok // (4 * experts * ep_size)
        assert (ep_size, tp_size, capacity, tok, experts) == (2, 4, MAIN + 4, 128, 32)
        n_main = experts * MAIN
        rows = SOURCES * capacity
        n_chunks = -(-d_model // WIDE)
        n_msg = FIRST_SUM + 5 * n_chunks
        vmem = pl.BlockSpec(memory_space=pltpu.VMEM)
        hbm = pl.BlockSpec(memory_space=pl.ANY)
        return pl.pallas_call(
            kernel,
            out_shape=jax.ShapeDtypeStruct((tok, d_model), BF16),
            in_specs=[vmem, vmem, hbm, hbm, hbm, hbm],
            out_specs=vmem,
            scratch_shapes=[
                pltpu.VMEM((SOURCES, tok, d_model), BF16),
                pltpu.VMEM((SOURCES, 2 * top_k, tok), F32),
                pltpu.VMEM((SOURCES, experts, tok), F32),
                pltpu.VMEM((4 * experts, 4 * n_main), BF16),
                pltpu.VMEM((SOURCES, 3 * tok, 2 * n_main), BF16),
                pltpu.VMEM((experts, rows, d_model), BF16),
                pltpu.VMEM((experts, rows, ff), BF16),
                pltpu.VMEM((RING, 2, d_model, ff), BF16),
                pltpu.VMEM((4, tok, d_model), F32),
                pltpu.VMEM((4, tok, d_model), F32),
                pltpu.VMEM((4, tok, d_model), F32),
                pltpu.VMEM((2, tok // 2, d_model), F32),
                pltpu.VMEM((2, tok // 2, d_model), F32),
                pltpu.VMEM((tok // 2, d_model), F32),
                pltpu.VMEM((tok // 2, d_model), F32),
                pltpu.VMEM((tok // 2, d_model), F32),
                pltpu.VMEM((tok // 2, d_model), F32),
                pltpu.SemaphoreType.DMA,
                pltpu.SemaphoreType.DMA((RING, 8)),
                pltpu.SemaphoreType.DMA((n_msg,)),
                pltpu.SemaphoreType.DMA((n_msg,)),
            ],
            compiler_params=pltpu.CompilerParams(
                collective_id=0, has_side_effects=True, vmem_limit_bytes=67043328
            ),
        )(expert_ids.T, gates.T, tokens, w_gate, w_up, w_down)

    return jax.shard_map(
        local_layer,
        mesh=mesh,
        in_specs=(row_spec, row_spec, row_spec, P("ep", None, "tp"), P("ep", None, "tp"), P("ep", "tp", None)),
        out_specs=row_spec,
        check_vma=False,
    )
```

```python
import functools

import jax
import jax.numpy as jnp
from jax import lax
from jax.experimental import pallas as pl
from jax.experimental.pallas import tpu as pltpu
from jax.sharding import PartitionSpec as P

MESH = pl.DeviceIdType.MESH
BF16 = jnp.bfloat16
F32 = jnp.float32

SOURCES = 8
MAIN = 16
BLOCK = 4
RING = 16
WIDE = 256
NO_SLOT = 255.0

META = range(8)
TO_PARTNER, X_LOW, X_HIGH, Y_HIGH, Y_LOW, DIAG_Y, DIAG_X, PASS_X, PASS_Y, PASS_D = range(8, 18)
FIRST_SUM = 18
OWN, XN, DIAG, YN = range(4)
PLACE = (OWN, XN, YN, DIAG)


def iota(shape, dim):
    return lax.broadcasted_iota(jnp.int32, shape, dim)


def kernel(
    ids_hbm, gates_hbm, tok_hbm, wg_hbm, wu_hbm, wd_hbm, out_hbm,
    ids_ref, gates_ref, xg, mg, val, spread, gmat, xe, yrest, ring, away, home, got, rx1, ry1, rx2, ry2, via_x, via_y, direct, result,
    own_sem, out_sem, wsem, ssem, rsem,
):
    top_k, tok = ids_hbm.shape
    experts = wg_hbm.shape[0]
    d_model, ff = wg_hbm.shape[1:]
    half = tok // 2
    rest = 4
    ep, tp = lax.axis_index("ep"), lax.axis_index("tp")
    other = tp + 1 - 2 * (tp % 2)
    tps = (tp, other, (tp + 2) % 4, (other + 2) % 4)
    device = [{"ep": ep if r < 4 else 1 - ep, "tp": tps[r % 4]} for r in range(SOURCES)]
    partner, xn, yn, diag = device[1], device[2], device[4], device[6]
    first_expert = ep * experts

    chunks = []
    start = 0
    while start < d_model:
        chunks.append((start, min(WIDE, d_model - start)))
        start += WIDE
    n_chunks = len(chunks)

    per_slot = 4
    groups = experts // per_slot

    def load_up(e, slot):
        return [
            pltpu.make_async_copy(wg_hbm.at[e], ring.at[slot, 0], wsem.at[slot]),
            pltpu.make_async_copy(wu_hbm.at[e], ring.at[slot, 1], wsem.at[slot]),
        ]

    def wait_up(slot):
        pltpu.make_async_copy(wg_hbm.at[pl.ds(0, 2)], ring.at[slot], wsem.at[slot]).wait()

    def wait_down(slot):
        area = pl.ds(0, ff), pl.ds(0, 2 * WIDE)
        pltpu.make_async_copy(wd_hbm.at[pl.ds(0, 2), *area], ring.at[slot, :, *area], wsem.at[slot]).wait()

    def down_view(slot, k, width):
        per_plane = 2 if width == WIDE else 4
        return ring.at[slot, k // per_plane, pl.ds(0, ff), pl.ds((k % per_plane) * width, width)]

    def load_down(first, column, width, slot):
        count = per_slot if width == WIDE else 2 * per_slot
        return [
            pltpu.make_async_copy(
                wd_hbm.at[first + k, :, pl.ds(column, width)], down_view(slot, k, width), wsem.at[slot]
            )
            for k in range(count)
        ]

    n_up = experts // BLOCK
    per_chunk = groups // BLOCK

    def down_block(b):
        lb = b - n_up
        c = lb // per_chunk if lb < per_chunk * (n_chunks - 1) else n_chunks - 1
        return c, (lb - c * per_chunk) * BLOCK * per_slot

    def start_down(b):
        c, first = down_block(b)
        column, width = chunks[c]
        step = per_slot if width == WIDE else 2 * per_slot
        for i in range(BLOCK):
            for copy in load_down(first + i * step, column, width, (b * BLOCK + i) % RING):
                copy.start()

    barrier = pltpu.get_barrier_semaphore()
    for dev in device[1:]:
        pl.semaphore_signal(barrier, inc=1, device_id=dev, device_id_type=MESH)
    mine = [
        pltpu.make_async_copy(ids_hbm, ids_ref, own_sem.at[0]),
        pltpu.make_async_copy(gates_hbm, gates_ref, own_sem.at[1]),
        pltpu.make_async_copy(tok_hbm, xg.at[0], own_sem.at[2]),
    ]
    for copy in mine:
        copy.start()

    def message(i, src, dst, dev):
        return pltpu.make_async_remote_copy(
            src_ref=src, dst_ref=dst, send_sem=ssem.at[i], recv_sem=rsem.at[i], device_id=dev, device_id_type=MESH
        )

    low, high = pl.ds(0, half), pl.ds(half, half)
    sent = {
        TO_PARTNER: message(TO_PARTNER, xg.at[0], xg.at[1], partner),
        X_LOW: message(X_LOW, xg.at[0, low], xg.at[2, low], xn),
        X_HIGH: message(X_HIGH, xg.at[0, high], xg.at[2, high], xn),
        Y_HIGH: message(Y_HIGH, xg.at[0, high], xg.at[4, high], yn),
        Y_LOW: message(Y_LOW, xg.at[0, low], xg.at[4, low], yn),
        DIAG_Y: message(DIAG_Y, xg.at[2, low], xg.at[6, low], yn),
        DIAG_X: message(DIAG_X, xg.at[4, high], xg.at[6, high], xn),
        PASS_X: message(PASS_X, xg.at[2], xg.at[3], partner),
        PASS_Y: message(PASS_Y, xg.at[4], xg.at[5], partner),
        PASS_D: message(PASS_D, xg.at[6], xg.at[7], partner),
    }

    for r in range(1, SOURCES):
        hop = r == 1 or r % 2 == 0
        sent[META[r]] = message(META[r], mg.at[0 if hop else r - 1], mg.at[r], device[r] if hop else partner)

    for copy in mine:
        copy.wait()
    mg[0, 0:top_k, :] = ids_ref[...].astype(F32)
    mg[0, top_k:, :] = gates_ref[...]
    for s in range(RING):
        for copy in load_up(s, s):
            copy.start()
    pl.semaphore_wait(barrier, SOURCES - 1)
    for r in (6, 2, 4, 1):
        sent[META[r]].start()
    for i in (X_LOW, Y_HIGH, X_HIGH, Y_LOW, TO_PARTNER):
        sent[i].start()

    earlier = jnp.where(iota((tok, tok), 0) < iota((tok, tok), 1), 1.0, 0.0).astype(BF16)
    expert_row = (iota((experts, tok), 0) + first_expert).astype(F32)
    n_main = experts * MAIN
    n_rest = experts * 2 * rest
    row, col = iota((4 * experts, 4 * n_main), 0), iota((4 * experts, 4 * n_main), 1)
    spread[:, 0 : 4 * n_main] = jnp.where(row == col // MAIN, 1.0, 0.0).astype(BF16)
    row, col = iota((4 * experts, 4 * n_rest), 0), iota((4 * experts, 4 * n_rest), 1)
    spread[:, 4 * n_main :] = jnp.where(row == col // (2 * rest), 1.0, 0.0).astype(BF16)

    def route(r):
        hit = jnp.zeros((experts, tok), F32)
        gate = jnp.zeros((experts, tok), F32)
        for j in range(top_k):
            here = mg[r, j : j + 1, :] == expert_row
            hit = jnp.where(here, 1.0, hit)
            gate = jnp.where(here, mg[r, top_k + j : top_k + j + 1, :], gate)
        before = jnp.dot(hit.astype(BF16), earlier, preferred_element_type=F32)
        slot = jnp.where(hit > 0.5, before, NO_SLOT)
        val[r] = slot
        g_hi = gate.astype(BF16).astype(F32)
        g_mid = (gate - g_hi).astype(BF16).astype(F32)
        g_lo = gate - g_hi - g_mid
        stack = jnp.concatenate([slot, g_hi, g_mid, g_lo], axis=0)
        by_token = stack.T.astype(BF16)
        wide = jnp.dot(by_token, spread[...], preferred_element_type=F32)
        lane = iota((tok, n_main), 1)
        in_main = wide[:, 0:n_main] == (lane % MAIN).astype(F32)
        lane = iota((tok, n_rest), 1)
        want = jnp.where(lane // rest % 2 == r % 2, MAIN + lane % rest, -1)
        in_rest = wide[:, 4 * n_main : 4 * n_main + n_rest] == want.astype(F32)
        for k in range(1, 4):
            rows = pl.ds((k - 1) * tok, tok)
            piece = wide[:, k * n_main : (k + 1) * n_main]
            gmat[r, rows, 0:n_main] = jnp.where(in_main, piece, 0.0).astype(BF16)
            piece = wide[:, 4 * n_main + k * n_rest : 4 * n_main + (k + 1) * n_rest]
            gmat[r, rows, n_main:] = jnp.where(in_rest, piece, 0.0).astype(BF16)

    def one_hot(slots, want, e):
        line = jnp.broadcast_to(slots[e : e + 1, :], want.shape)
        return jnp.where(line == want, 1.0, 0.0).astype(BF16)

    def dispatch(sources, want, rows, batch):
        slots = jnp.concatenate([val[r] for r in sources], axis=1)
        x = xg[sources[0] : sources[-1] + 1].reshape(len(sources) * tok, d_model)
        height = want.shape[0]
        for e in range(0, experts, batch):
            pick = jnp.concatenate([one_hot(slots, want, e + i) for i in range(batch)], axis=0)
            placed = jnp.dot(pick, x, preferred_element_type=F32).astype(BF16)
            xe[e : e + batch, rows : rows + height, :] = placed.reshape(batch, height, d_model)

    def dispatch_pair(p):
        shape = (2 * MAIN, 2 * tok)
        i, l = iota(shape, 0), iota(shape, 1)
        want = jnp.where(i // MAIN == l // tok, i % MAIN, -1).astype(F32)
        dispatch([2 * p, 2 * p + 1], want, 2 * MAIN * p, 8)

    def dispatch_rest(q):
        shape = (4 * rest, 4 * tok)
        i, l = iota(shape, 0), iota(shape, 1)
        want = jnp.where(i // rest == l // tok, MAIN + i % rest, -1).astype(F32)
        dispatch([4 * q + i for i in range(4)], want, MAIN * SOURCES + 4 * rest * q, 16)

    def route_range(lo, hi):
        @pl.loop(lo, hi)
        def _(r):
            route(r)

    route_range(0, 1)
    sent[META[1]].wait_recv()
    route_range(1, 2)
    sent[TO_PARTNER].wait_recv()
    dispatch_pair(0)
    for r in range(2, SOURCES, 2):
        sent[META[r]].wait_recv()
        sent[META[r + 1]].start()
    for r in range(3, SOURCES, 2):
        sent[META[r]].wait_recv()
    route_range(2, 5)
    sent[X_LOW].wait_recv()
    sent[DIAG_Y].start()
    sent[Y_HIGH].wait_recv()
    sent[DIAG_X].start()
    route_range(5, 8)
    sent[X_HIGH].wait_recv()
    sent[PASS_X].start()
    sent[Y_LOW].wait_recv()
    sent[PASS_Y].start()
    sent[PASS_X].wait_recv()
    dispatch_pair(1)
    sent[PASS_Y].wait_recv()
    dispatch_pair(2)
    sent[DIAG_Y].wait_recv()
    sent[DIAG_X].wait_recv()
    sent[PASS_D].start()
    dispatch_rest(0)
    sent[PASS_D].wait_recv()
    dispatch_pair(3)
    dispatch_rest(1)

    full = ff // WIDE * WIDE

    def up_block(b):
        base = (b * BLOCK) % RING
        for i in range(BLOCK):
            wait_up(base + i)
        for i in range(BLOCK):
            e, slot = b * BLOCK + i, base + i
            x = xe[e]
            a = jnp.dot(x, ring[slot, 0, :, 0:full], preferred_element_type=F32)
            u = jnp.dot(x, ring[slot, 1, :, 0:full], preferred_element_type=F32)
            xe[e, :, 0:full] = (jax.nn.silu(a) * u).astype(BF16)
            tail = jnp.concatenate([ring[slot, 0, :, full:], ring[slot, 1, :, full:]], axis=1)
            t = jnp.dot(x, tail, preferred_element_type=F32)
            xe[e, :, full:ff] = (jax.nn.silu(t[:, : ff - full]) * t[:, ff - full :]).astype(BF16)

    ahead = RING // BLOCK

    for b in range(n_up):
        up_block(b)
        if b + ahead < n_up:
            for i in range(BLOCK):
                for copy in load_up((b + ahead) * BLOCK + i, (b * BLOCK) % RING + i):
                    copy.start()
        else:
            start_down(b + ahead)

    n_blocks = n_up + per_chunk * (n_chunks - 1) + 1

    def down(b, lo, hi):
        c, first = down_block(b)
        column, width = chunks[c]
        step = per_slot if width == WIDE else 2 * per_slot
        for i in range(lo, hi):
            wait_down((b * BLOCK + i) % RING)
        for i in range(lo, hi):
            for k in range(step):
                e = first + i * step + k
                w = down_view((b * BLOCK + i) % RING, k, width)[...]
                y = jnp.dot(xe[e, :, 0:ff], w, preferred_element_type=F32)
                xe[e, 0 : MAIN * SOURCES, ff : ff + width] = y[0 : MAIN * SOURCES].astype(BF16)
                yrest[e, :, 0:width] = y[MAIN * SOURCES :]
        if hi == BLOCK and b + ahead < n_blocks:
            start_down(b + ahead)

    def gated(r, c):
        width = chunks[c][1]
        top, bottom = MAIN * r, 2 * rest * (r // 2)
        y = jnp.concatenate(
            [
                xe[:, top : top + MAIN, ff : ff + width].reshape(n_main, width),
                yrest[:, bottom : bottom + 2 * rest, 0:width].reshape(n_rest, width).astype(BF16),
            ],
            axis=0,
        )
        s = jnp.dot(gmat[r], y, preferred_element_type=F32)
        return s[0:tok] + s[tok : 2 * tok] + s[2 * tok :]

    def cols(c):
        return pl.ds(*chunks[c])

    last = n_chunks - 1

    def sums(kind, c):
        i = FIRST_SUM + 5 * c + kind
        if kind == 0:
            return message(i, away.at[:, :, cols(c)], got.at[:, :, cols(c)], partner)
        if c == last:
            place, dev = ((XN, xn), (YN, yn), (DIAG, diag))[kind - 1]
            return message(i, home.at[place, :, cols(c)], direct.at[kind - 1], dev)
        if kind == 1:
            return message(i, home.at[pl.ds(XN, 2), low, cols(c)], rx1.at[:, :, cols(c)], xn)
        if kind == 2:
            return message(i, home.at[pl.ds(DIAG, 2), high, cols(c)], ry1.at[:, :, cols(c)], yn)
        if kind == 3:
            return message(i, via_y.at[:, cols(c)], ry2.at[:, cols(c)], yn)
        return message(i, via_x.at[:, cols(c)], rx2.at[:, cols(c)], xn)

    def combine_away(c):
        for r in range(1, SOURCES, 2):
            away[PLACE[r // 2], :, cols(c)] = gated(r, c)

    def combine_home(c):
        sums(0, c).start()
        for r in range(0, SOURCES, 2):
            home[PLACE[r // 2], :, cols(c)] = gated(r, c)

    def chip_sum(c):
        sums(0, c).wait_recv()
        for d in range(4):
            home[d, :, cols(c)] += got[d, :, cols(c)]
        for kind in (3, 1, 2) if c == last else (1, 2):
            sums(kind, c).start()

    def pass_on(c):
        sums(1, c).wait_recv()
        via_y[:, cols(c)] = home[YN, low, cols(c)] + rx1[1, :, cols(c)]
        sums(3, c).start()
        sums(2, c).wait_recv()
        via_x[:, cols(c)] = home[XN, high, cols(c)] + ry1[0, :, cols(c)]
        sums(4, c).start()

    def write(c):
        return pltpu.make_async_copy(result.at[:, cols(c)], out_hbm.at[:, cols(c)], out_sem.at[c])

    def finish(c):
        if c == last:
            total = home[OWN, :, cols(c)]
            for kind in (1, 2, 3):
                sums(kind, c).wait_recv()
                total += direct[kind - 1]
            result[:, cols(c)] = total.astype(BF16)
        else:
            sums(3, c).wait_recv()
            result[low, cols(c)] = (home[OWN, low, cols(c)] + rx1[0, :, cols(c)] + ry2[:, cols(c)]).astype(BF16)
            sums(4, c).wait_recv()
            result[high, cols(c)] = (home[OWN, high, cols(c)] + ry1[1, :, cols(c)] + rx2[:, cols(c)]).astype(BF16)
        write(c).start()

    b = n_up
    for c in range(n_chunks):
        if c < n_chunks - 1:
            parts = [(b, 0, BLOCK // 2), (b, BLOCK // 2, BLOCK)] + [(b + i, 0, BLOCK) for i in range(1, per_chunk)]
            b += per_chunk
        else:
            parts = [(b, 0, BLOCK // 2), (b, BLOCK // 2, BLOCK)]
        for n, part in enumerate(parts):
            down(*part)
            if n == 0 and c >= 1:
                chip_sum(c - 1)
            if n == 1 and c >= 2:
                pass_on(c - 2)
        combine_away(c)
        combine_home(c)
    finish(0)
    chip_sum(last)
    pass_on(last - 1)
    for c in range(1, last - 1):
        finish(c)
    finish(last)
    finish(last - 1)

    for i in range(1, FIRST_SUM):
        sent[i].wait_send()
    for c in range(n_chunks):
        for kind in range(4 if c == last else 5):
            sums(kind, c).wait_send()
        write(c).wait()


def solution(mesh):
    ep_size, tp_size = mesh.shape["ep"], mesh.shape["tp"]
    row_spec = P(("dp", "ep", "tp"), None)

    def local_layer(tokens, expert_ids, gates, w_gate, w_up, w_down):
        tok, d_model = tokens.shape
        top_k = expert_ids.shape[1]
        experts, _, ff = w_gate.shape
        capacity = 5 * top_k * tok // (4 * experts * ep_size)
        assert (ep_size, tp_size, capacity, tok, experts) == (2, 4, MAIN + 4, 128, 32)
        n_main, n_rest = experts * MAIN, experts * 8
        rows = SOURCES * capacity
        n_chunks = -(-d_model // WIDE)
        n_msg = FIRST_SUM + 5 * n_chunks
        hbm = pl.BlockSpec(memory_space=pl.ANY)
        return pl.pallas_call(
            kernel,
            out_shape=jax.ShapeDtypeStruct((tok, d_model), BF16),
            in_specs=[hbm] * 6,
            out_specs=hbm,
            scratch_shapes=[
                pltpu.VMEM((top_k, tok), jnp.int32),
                pltpu.VMEM((top_k, tok), F32),
                pltpu.VMEM((SOURCES, tok, d_model), BF16),
                pltpu.VMEM((SOURCES, 2 * top_k, tok), F32),
                pltpu.VMEM((SOURCES, experts, tok), F32),
                pltpu.VMEM((4 * experts, 4 * (n_main + n_rest)), BF16),
                pltpu.VMEM((SOURCES, 3 * tok, n_main + n_rest), BF16),
                pltpu.VMEM((experts, rows, d_model), BF16),
                pltpu.VMEM((experts, rows - MAIN * SOURCES, WIDE), F32),
                pltpu.VMEM((RING, 2, d_model, ff), BF16),
                pltpu.VMEM((4, tok, d_model), F32),
                pltpu.VMEM((4, tok, d_model), F32),
                pltpu.VMEM((4, tok, d_model), F32),
                pltpu.VMEM((2, tok // 2, d_model), F32),
                pltpu.VMEM((2, tok // 2, d_model), F32),
                pltpu.VMEM((tok // 2, d_model), F32),
                pltpu.VMEM((tok // 2, d_model), F32),
                pltpu.VMEM((tok // 2, d_model), F32),
                pltpu.VMEM((tok // 2, d_model), F32),
                pltpu.VMEM((3, tok, d_model - WIDE * (n_chunks - 1)), F32),
                pltpu.VMEM((tok, d_model), BF16),
                pltpu.SemaphoreType.DMA((3,)),
                pltpu.SemaphoreType.DMA((n_chunks,)),
                pltpu.SemaphoreType.DMA((RING,)),
                pltpu.SemaphoreType.DMA((n_msg,)),
                pltpu.SemaphoreType.DMA((n_msg,)),
            ],
            compiler_params=pltpu.CompilerParams(
                collective_id=0, has_side_effects=True, vmem_limit_bytes=67043328
            ),
        )(expert_ids.T, gates.T, tokens, w_gate, w_up, w_down)

    return jax.shard_map(
        local_layer,
        mesh=mesh,
        in_specs=(row_spec, row_spec, row_spec, P("ep", None, "tp"), P("ep", None, "tp"), P("ep", "tp", None)),
        out_specs=row_spec,
        check_vma=False,
    )
```

```python
import functools

import jax
import jax.numpy as jnp
from jax import lax
from jax.experimental import pallas as pl
from jax.experimental.pallas import tpu as pltpu
from jax.sharding import PartitionSpec as P

MESH = pl.DeviceIdType.MESH
BF16 = jnp.bfloat16
F32 = jnp.float32

SOURCES = 8
MAIN = 16
BLOCK = 4
RING = 16
WIDE = 256
NO_SLOT = 255.0

META = range(8)
TO_PARTNER, X_LOW, X_HIGH, Y_HIGH, Y_LOW, DIAG_Y, DIAG_X, PASS_X, PASS_Y, PASS_D = range(8, 18)
FIRST_SUM = 18
OWN, XN, DIAG, YN = range(4)
PLACE = (OWN, XN, YN, DIAG)


def iota(shape, dim):
    return lax.broadcasted_iota(jnp.int32, shape, dim)


def kernel(
    ids_hbm, gates_hbm, tok_hbm, wg_hbm, wu_hbm, wd_hbm, out_hbm,
    ids_ref, gates_ref, xg, mg, val, spread, gmat, xe, yrest, ring, away, home, got, rx1, ry1, rx2, ry2, via_x, via_y, direct, result,
    own_sem, out_sem, wsem, ssem, rsem,
):
    top_k, tok = ids_hbm.shape
    experts = wg_hbm.shape[0]
    d_model, ff = wg_hbm.shape[1:]
    half = tok // 2
    rest = 4
    ep, tp = lax.axis_index("ep"), lax.axis_index("tp")
    other = tp + 1 - 2 * (tp % 2)
    tps = (tp, other, (tp + 2) % 4, (other + 2) % 4)
    device = [{"ep": ep if r < 4 else 1 - ep, "tp": tps[r % 4]} for r in range(SOURCES)]
    partner, xn, yn, diag = device[1], device[2], device[4], device[6]
    first_expert = ep * experts

    chunks = []
    start = 0
    while start < d_model:
        chunks.append((start, min(WIDE, d_model - start)))
        start += WIDE
    n_chunks = len(chunks)

    per_slot = 4
    groups = experts // per_slot

    def load_up(e, slot):
        return [
            pltpu.make_async_copy(wg_hbm.at[e], ring.at[slot, 0], wsem.at[slot]),
            pltpu.make_async_copy(wu_hbm.at[e], ring.at[slot, 1], wsem.at[slot]),
        ]

    def wait_up(slot):
        pltpu.make_async_copy(wg_hbm.at[pl.ds(0, 2)], ring.at[slot], wsem.at[slot]).wait()

    def wait_down(slot):
        area = pl.ds(0, ff), pl.ds(0, 2 * WIDE)
        pltpu.make_async_copy(wd_hbm.at[pl.ds(0, 2), *area], ring.at[slot, :, *area], wsem.at[slot]).wait()

    def down_view(slot, k, width):
        per_plane = 2 if width == WIDE else 4
        return ring.at[slot, k // per_plane, pl.ds(0, ff), pl.ds((k % per_plane) * width, width)]

    def load_down(first, column, width, slot):
        count = per_slot if width == WIDE else 2 * per_slot
        return [
            pltpu.make_async_copy(
                wd_hbm.at[first + k, :, pl.ds(column, width)], down_view(slot, k, width), wsem.at[slot]
            )
            for k in range(count)
        ]

    n_up = experts // BLOCK
    per_chunk = groups // BLOCK

    def down_block(b):
        lb = b - n_up
        c = lb // per_chunk if lb < per_chunk * (n_chunks - 1) else n_chunks - 1
        return c, (lb - c * per_chunk) * BLOCK * per_slot

    def start_down(b):
        c, first = down_block(b)
        column, width = chunks[c]
        step = per_slot if width == WIDE else 2 * per_slot
        for i in range(BLOCK):
            for copy in load_down(first + i * step, column, width, (b * BLOCK + i) % RING):
                copy.start()

    barrier = pltpu.get_barrier_semaphore()
    for dev in device[1:]:
        pl.semaphore_signal(barrier, inc=1, device_id=dev, device_id_type=MESH)
    mine = [
        pltpu.make_async_copy(ids_hbm, ids_ref, own_sem.at[0]),
        pltpu.make_async_copy(gates_hbm, gates_ref, own_sem.at[1]),
        pltpu.make_async_copy(tok_hbm, xg.at[0], own_sem.at[2]),
    ]
    for copy in mine:
        copy.start()

    def message(i, src, dst, dev):
        return pltpu.make_async_remote_copy(
            src_ref=src, dst_ref=dst, send_sem=ssem.at[i], recv_sem=rsem.at[i], device_id=dev, device_id_type=MESH
        )

    low, high = pl.ds(0, half), pl.ds(half, half)
    sent = {
        TO_PARTNER: message(TO_PARTNER, xg.at[0], xg.at[1], partner),
        X_LOW: message(X_LOW, xg.at[0, low], xg.at[2, low], xn),
        X_HIGH: message(X_HIGH, xg.at[0, high], xg.at[2, high], xn),
        Y_HIGH: message(Y_HIGH, xg.at[0, high], xg.at[4, high], yn),
        Y_LOW: message(Y_LOW, xg.at[0, low], xg.at[4, low], yn),
        DIAG_Y: message(DIAG_Y, xg.at[2, low], xg.at[6, low], yn),
        DIAG_X: message(DIAG_X, xg.at[4, high], xg.at[6, high], xn),
        PASS_X: message(PASS_X, xg.at[2], xg.at[3], partner),
        PASS_Y: message(PASS_Y, xg.at[4], xg.at[5], partner),
        PASS_D: message(PASS_D, xg.at[6], xg.at[7], partner),
    }

    for r in range(1, SOURCES):
        hop = r == 1 or r % 2 == 0
        sent[META[r]] = message(META[r], mg.at[0 if hop else r - 1], mg.at[r], device[r] if hop else partner)

    for copy in mine:
        copy.wait()
    mg[0, 0:top_k, :] = ids_ref[...].astype(F32)
    mg[0, top_k:, :] = gates_ref[...]
    for s in range(RING):
        for copy in load_up(s, s):
            copy.start()
    pl.semaphore_wait(barrier, SOURCES - 1)
    for r in (6, 2, 4, 1):
        sent[META[r]].start()
    for i in (X_LOW, Y_HIGH, X_HIGH, Y_LOW, TO_PARTNER):
        sent[i].start()

    earlier = jnp.where(iota((tok, tok), 0) < iota((tok, tok), 1), 1.0, 0.0).astype(BF16)
    expert_row = (iota((experts, tok), 0) + first_expert).astype(F32)
    n_main = experts * MAIN
    n_rest = experts * 2 * rest
    row, col = iota((4 * experts, 4 * n_main), 0), iota((4 * experts, 4 * n_main), 1)
    spread[:, 0 : 4 * n_main] = jnp.where(row == col // MAIN, 1.0, 0.0).astype(BF16)
    row, col = iota((4 * experts, 4 * n_rest), 0), iota((4 * experts, 4 * n_rest), 1)
    spread[:, 4 * n_main :] = jnp.where(row == col // (2 * rest), 1.0, 0.0).astype(BF16)

    def route(r):
        hit = jnp.zeros((experts, tok), F32)
        gate = jnp.zeros((experts, tok), F32)
        for j in range(top_k):
            here = mg[r, j : j + 1, :] == expert_row
            hit = jnp.where(here, 1.0, hit)
            gate = jnp.where(here, mg[r, top_k + j : top_k + j + 1, :], gate)
        before = jnp.dot(hit.astype(BF16), earlier, preferred_element_type=F32)
        slot = jnp.where(hit > 0.5, before, NO_SLOT)
        val[r] = slot
        g_hi = gate.astype(BF16).astype(F32)
        g_mid = (gate - g_hi).astype(BF16).astype(F32)
        g_lo = gate - g_hi - g_mid
        stack = jnp.concatenate([slot, g_hi, g_mid, g_lo], axis=0)
        by_token = stack.T.astype(BF16)
        wide = jnp.dot(by_token, spread[...], preferred_element_type=F32)
        lane = iota((tok, n_main), 1)
        in_main = wide[:, 0:n_main] == (lane % MAIN).astype(F32)
        lane = iota((tok, n_rest), 1)
        want = jnp.where(lane // rest % 2 == r % 2, MAIN + lane % rest, -1)
        in_rest = wide[:, 4 * n_main : 4 * n_main + n_rest] == want.astype(F32)
        for k in range(1, 4):
            rows = pl.ds((k - 1) * tok, tok)
            piece = wide[:, k * n_main : (k + 1) * n_main]
            gmat[r, rows, 0:n_main] = jnp.where(in_main, piece, 0.0).astype(BF16)
            piece = wide[:, 4 * n_main + k * n_rest : 4 * n_main + (k + 1) * n_rest]
            gmat[r, rows, n_main:] = jnp.where(in_rest, piece, 0.0).astype(BF16)

    def one_hot(slots, want, e):
        line = jnp.broadcast_to(slots[e : e + 1, :], want.shape)
        return jnp.where(line == want, 1.0, 0.0).astype(BF16)

    def dispatch(sources, want, rows, batch, held=None):
        slots = jnp.concatenate([val[r] for r in sources], axis=1) if len(sources) > 1 else val[sources[0]]
        x = xg[sources[0] : sources[-1] + 1].reshape(len(sources) * tok, d_model)
        height = want.shape[0]
        for e in range(0, experts, batch):
            pick = jnp.concatenate([one_hot(slots, want, e + i) for i in range(batch)], axis=0)
            placed = jnp.dot(pick, x, preferred_element_type=F32)
            part = slice(e * height // tok, (e + batch) * height // tok)
            if held == "keep":
                away[part] = placed.reshape(-1, tok, d_model)
                continue
            if held == "add":
                placed += away[part].reshape(placed.shape)
            xe[e : e + batch, rows : rows + height, :] = placed.astype(BF16).reshape(batch, height, d_model)

    def dispatch_main(*sources):
        shape = (len(sources) * MAIN, len(sources) * tok)
        i, l = iota(shape, 0), iota(shape, 1)
        want = jnp.where(i // MAIN == l // tok, i % MAIN, -1).astype(F32)
        dispatch(sources, want, MAIN * sources[0], 16 // len(sources))

    def dispatch_rest(sources, held=None):
        q = sources[0] // 4
        shape = (4 * rest, len(sources) * tok)
        i, l = iota(shape, 0), iota(shape, 1)
        want = jnp.where(4 * q + i // rest == sources[0] + l // tok, MAIN + i % rest, -1).astype(F32)
        dispatch(sources, want, MAIN * SOURCES + 4 * rest * q, 16, held)

    def route_range(lo, hi):
        @pl.loop(lo, hi)
        def _(r):
            route(r)

    route_range(0, 1)
    sent[META[1]].wait_recv()
    route_range(1, 2)
    sent[TO_PARTNER].wait_recv()
    dispatch_main(0, 1)
    for r in range(2, SOURCES, 2):
        sent[META[r]].wait_recv()
        sent[META[r + 1]].start()
    for r in range(3, SOURCES, 2):
        sent[META[r]].wait_recv()
    route_range(2, 5)
    sent[X_LOW].wait_recv()
    sent[DIAG_Y].start()
    sent[Y_HIGH].wait_recv()
    sent[DIAG_X].start()
    route_range(5, 8)
    sent[X_HIGH].wait_recv()
    sent[PASS_X].start()
    sent[Y_LOW].wait_recv()
    sent[PASS_Y].start()
    dispatch_main(2)
    dispatch_main(4)
    sent[PASS_X].wait_recv()
    dispatch_main(3)
    sent[PASS_Y].wait_recv()
    dispatch_main(5)
    dispatch_rest((0, 1, 2, 3))
    sent[DIAG_Y].wait_recv()
    sent[DIAG_X].wait_recv()
    sent[PASS_D].start()
    dispatch_rest((4, 5), "keep")
    dispatch_main(6)
    sent[PASS_D].wait_recv()
    dispatch_main(7)
    dispatch_rest((6, 7), "add")

    full = ff // WIDE * WIDE

    def up_block(b):
        base = (b * BLOCK) % RING
        for i in range(BLOCK):
            wait_up(base + i)
        for i in range(BLOCK):
            e, slot = b * BLOCK + i, base + i
            x = xe[e]
            a = jnp.dot(x, ring[slot, 0, :, 0:full], preferred_element_type=F32)
            u = jnp.dot(x, ring[slot, 1, :, 0:full], preferred_element_type=F32)
            xe[e, :, 0:full] = (jax.nn.silu(a) * u).astype(BF16)
            tail = jnp.concatenate([ring[slot, 0, :, full:], ring[slot, 1, :, full:]], axis=1)
            t = jnp.dot(x, tail, preferred_element_type=F32)
            xe[e, :, full:ff] = (jax.nn.silu(t[:, : ff - full]) * t[:, ff - full :]).astype(BF16)

    ahead = RING // BLOCK

    for b in range(n_up):
        up_block(b)
        if b + ahead < n_up:
            for i in range(BLOCK):
                for copy in load_up((b + ahead) * BLOCK + i, (b * BLOCK) % RING + i):
                    copy.start()
        else:
            start_down(b + ahead)

    def wait_block(b, lo=0, hi=BLOCK):
        for i in range(lo, hi):
            wait_down((b * BLOCK + i) % RING)

    n_blocks = n_up + per_chunk * (n_chunks - 1) + 1

    def down(b, lo, hi):
        c, first = down_block(b)
        column, width = chunks[c]
        step = per_slot if width == WIDE else 2 * per_slot
        for i in range(lo, hi):
            for k in range(step):
                e = first + i * step + k
                w = down_view((b * BLOCK + i) % RING, k, width)[...]
                y = jnp.dot(xe[e, :, 0:ff], w, preferred_element_type=F32)
                xe[e, 0 : MAIN * SOURCES, ff : ff + width] = y[0 : MAIN * SOURCES].astype(BF16)
                yrest[e, :, 0:width] = y[MAIN * SOURCES :]
        if hi == BLOCK and b + ahead < n_blocks:
            start_down(b + ahead)

    def gated(r, c):
        width = chunks[c][1]
        top, bottom = MAIN * r, 2 * rest * (r // 2)
        y = jnp.concatenate(
            [
                xe[:, top : top + MAIN, ff : ff + width].reshape(n_main, width),
                yrest[:, bottom : bottom + 2 * rest, 0:width].reshape(n_rest, width).astype(BF16),
            ],
            axis=0,
        )
        s = jnp.dot(gmat[r], y, preferred_element_type=F32)
        return s[0:tok] + s[tok : 2 * tok] + s[2 * tok :]

    def cols(c):
        return pl.ds(*chunks[c])

    last = n_chunks - 1

    def sums(kind, c):
        i = FIRST_SUM + 5 * c + kind
        if kind == 0:
            return message(i, away.at[:, :, cols(c)], got.at[:, :, cols(c)], partner)
        if c == last:
            place, dev = ((XN, xn), (YN, yn), (DIAG, diag))[kind - 1]
            return message(i, home.at[place, :, cols(c)], direct.at[kind - 1], dev)
        if kind == 1:
            return message(i, home.at[pl.ds(XN, 2), low, cols(c)], rx1.at[:, :, cols(c)], xn)
        if kind == 2:
            return message(i, home.at[pl.ds(DIAG, 2), high, cols(c)], ry1.at[:, :, cols(c)], yn)
        if kind == 3:
            return message(i, via_y.at[:, cols(c)], ry2.at[:, cols(c)], yn)
        return message(i, via_x.at[:, cols(c)], rx2.at[:, cols(c)], xn)

    def combine_away(c):
        for r in range(1, SOURCES, 2):
            away[PLACE[r // 2], :, cols(c)] = gated(r, c)

    def combine_home(c):
        sums(0, c).start()
        for r in range(0, SOURCES, 2):
            home[PLACE[r // 2], :, cols(c)] = gated(r, c)

    def chip_sum(c):
        sums(0, c).wait_recv()
        for d in range(4):
            home[d, :, cols(c)] += got[d, :, cols(c)]
        for kind in (3, 1, 2) if c == last else (1, 2):
            sums(kind, c).start()

    def pass_on(c):
        sums(1, c).wait_recv()
        via_y[:, cols(c)] = home[YN, low, cols(c)] + rx1[1, :, cols(c)]
        sums(3, c).start()
        sums(2, c).wait_recv()
        via_x[:, cols(c)] = home[XN, high, cols(c)] + ry1[0, :, cols(c)]
        sums(4, c).start()

    def write(c):
        return pltpu.make_async_copy(result.at[:, cols(c)], out_hbm.at[:, cols(c)], out_sem.at[c])

    def finish(c):
        if c == last:
            total = home[OWN, :, cols(c)]
            for kind in (1, 2, 3):
                sums(kind, c).wait_recv()
                total += direct[kind - 1]
            result[:, cols(c)] = total.astype(BF16)
        else:
            sums(3, c).wait_recv()
            result[low, cols(c)] = (home[OWN, low, cols(c)] + rx1[0, :, cols(c)] + ry2[:, cols(c)]).astype(BF16)
            sums(4, c).wait_recv()
            result[high, cols(c)] = (home[OWN, high, cols(c)] + ry1[1, :, cols(c)] + rx2[:, cols(c)]).astype(BF16)
        write(c).start()

    def blocks(c):
        return range(n_up + c * per_chunk, min(n_up + (c + 1) * per_chunk, n_blocks))

    for c in range(n_chunks):
        first, *others = blocks(c)
        if c == 0:
            wait_block(first)
            down(first, 0, BLOCK)
        else:
            cut = BLOCK // 2 if c < last else BLOCK // 4
            wait_block(first, 0, cut)
            down(first, 0, cut)
            chip_sum(c - 1)
            wait_block(first, cut, BLOCK)
            for b in others:
                wait_block(b)
            down(first, cut, BLOCK)
        for b in others:
            if c == 0:
                wait_block(b)
            down(b, 0, BLOCK)
        if c >= 2:
            pass_on(c - 2)
        combine_away(c)
        combine_home(c)
    finish(0)
    chip_sum(last)
    pass_on(last - 1)
    for c in range(1, last - 1):
        finish(c)
    finish(last)
    finish(last - 1)

    for i in range(1, FIRST_SUM):
        sent[i].wait_send()
    for c in range(n_chunks):
        for kind in range(4 if c == last else 5):
            sums(kind, c).wait_send()
        write(c).wait()


def solution(mesh):
    ep_size, tp_size = mesh.shape["ep"], mesh.shape["tp"]
    row_spec = P(("dp", "ep", "tp"), None)

    def local_layer(tokens, expert_ids, gates, w_gate, w_up, w_down):
        tok, d_model = tokens.shape
        top_k = expert_ids.shape[1]
        experts, _, ff = w_gate.shape
        capacity = 5 * top_k * tok // (4 * experts * ep_size)
        assert (ep_size, tp_size, capacity, tok, experts) == (2, 4, MAIN + 4, 128, 32)
        n_main, n_rest = experts * MAIN, experts * 8
        rows = SOURCES * capacity
        n_chunks = -(-d_model // WIDE)
        n_msg = FIRST_SUM + 5 * n_chunks
        hbm = pl.BlockSpec(memory_space=pl.ANY)
        return pl.pallas_call(
            kernel,
            out_shape=jax.ShapeDtypeStruct((tok, d_model), BF16),
            in_specs=[hbm] * 6,
            out_specs=hbm,
            scratch_shapes=[
                pltpu.VMEM((top_k, tok), jnp.int32),
                pltpu.VMEM((top_k, tok), F32),
                pltpu.VMEM((SOURCES, tok, d_model), BF16),
                pltpu.VMEM((SOURCES, 2 * top_k, tok), F32),
                pltpu.VMEM((SOURCES, experts, tok), F32),
                pltpu.VMEM((4 * experts, 4 * (n_main + n_rest)), BF16),
                pltpu.VMEM((SOURCES, 3 * tok, n_main + n_rest), BF16),
                pltpu.VMEM((experts, rows, d_model), BF16),
                pltpu.VMEM((experts, rows - MAIN * SOURCES, WIDE), F32),
                pltpu.VMEM((RING, 2, d_model, ff), BF16),
                pltpu.VMEM((4, tok, d_model), F32),
                pltpu.VMEM((4, tok, d_model), F32),
                pltpu.VMEM((4, tok, d_model), F32),
                pltpu.VMEM((2, tok // 2, d_model), F32),
                pltpu.VMEM((2, tok // 2, d_model), F32),
                pltpu.VMEM((tok // 2, d_model), F32),
                pltpu.VMEM((tok // 2, d_model), F32),
                pltpu.VMEM((tok // 2, d_model), F32),
                pltpu.VMEM((tok // 2, d_model), F32),
                pltpu.VMEM((3, tok, d_model - WIDE * (n_chunks - 1)), F32),
                pltpu.VMEM((tok, d_model), BF16),
                pltpu.SemaphoreType.DMA((3,)),
                pltpu.SemaphoreType.DMA((n_chunks,)),
                pltpu.SemaphoreType.DMA((RING,)),
                pltpu.SemaphoreType.DMA((n_msg,)),
                pltpu.SemaphoreType.DMA((n_msg,)),
            ],
            compiler_params=pltpu.CompilerParams(
                collective_id=0, has_side_effects=True, vmem_limit_bytes=67043328
            ),
        )(expert_ids.T, gates.T, tokens, w_gate, w_up, w_down)

    return jax.shard_map(
        local_layer,
        mesh=mesh,
        in_specs=(row_spec, row_spec, row_spec, P("ep", None, "tp"), P("ep", None, "tp"), P("ep", "tp", None)),
        out_specs=row_spec,
        check_vma=False,
    )
```

```python
import functools

import jax
import jax.numpy as jnp
from jax import lax
from jax.experimental import pallas as pl
from jax.experimental.pallas import tpu as pltpu
from jax.sharding import PartitionSpec as P

MESH = pl.DeviceIdType.MESH
BF16 = jnp.bfloat16
F32 = jnp.float32

SOURCES = 8
MAIN = 16
BLOCK = 4
RING = 16
WIDE = 256
NO_SLOT = 255.0

META = range(8)
TO_PARTNER, X_LOW, X_HIGH, Y_HIGH, Y_LOW, DIAG_Y, DIAG_X, PASS_X, PASS_Y, PASS_D = range(8, 18)
FIRST_SUM = 18
META_SENT, ROWS_SENT, SUM_SENT, LAST_SENT = 0, 1, 2, 7
OWN, XN, DIAG, YN = range(4)
PLACE = (OWN, XN, YN, DIAG)


def iota(shape, dim):
    return lax.broadcasted_iota(jnp.int32, shape, dim)


def kernel(
    ids_hbm, gates_hbm, tok_hbm, wg_hbm, wu_hbm, wd_hbm, out_hbm,
    ids_ref, gates_ref, xg, mg, val, spread, gmat, xe, yrest, ring, away, home, got, rx1, ry1, rx2, ry2, via_x, via_y, direct, result,
    own_sem, out_sem, wsem, ssem, rsem,
):
    top_k, tok = ids_hbm.shape
    experts = wg_hbm.shape[0]
    d_model, ff = wg_hbm.shape[1:]
    half = tok // 2
    rest = 4
    ep, tp = lax.axis_index("ep"), lax.axis_index("tp")
    other = tp + 1 - 2 * (tp % 2)
    tps = (tp, other, (tp + 2) % 4, (other + 2) % 4)
    device = [{"ep": ep if r < 4 else 1 - ep, "tp": tps[r % 4]} for r in range(SOURCES)]
    partner, xn, yn, diag = device[1], device[2], device[4], device[6]
    first_expert = ep * experts

    chunks = []
    start = 0
    while start < d_model:
        chunks.append((start, min(WIDE, d_model - start)))
        start += WIDE
    n_chunks = len(chunks)

    per_slot = 4
    groups = experts // per_slot

    def load_up(e, slot):
        return [
            pltpu.make_async_copy(wg_hbm.at[e], ring.at[slot, 0], wsem.at[slot]),
            pltpu.make_async_copy(wu_hbm.at[e], ring.at[slot, 1], wsem.at[slot]),
        ]

    def wait_up(slot):
        pltpu.make_async_copy(wg_hbm.at[pl.ds(0, 2)], ring.at[slot], wsem.at[slot]).wait()

    def wait_down(slot):
        area = pl.ds(0, ff), pl.ds(0, 2 * WIDE)
        pltpu.make_async_copy(wd_hbm.at[pl.ds(0, 2), *area], ring.at[slot, :, *area], wsem.at[slot]).wait()

    def down_view(slot, k, width):
        per_plane = 2 if width == WIDE else 4
        return ring.at[slot, k // per_plane, pl.ds(0, ff), pl.ds((k % per_plane) * width, width)]

    def load_down(first, column, width, slot):
        count = per_slot if width == WIDE else 2 * per_slot
        return [
            pltpu.make_async_copy(
                wd_hbm.at[first + k, :, pl.ds(column, width)], down_view(slot, k, width), wsem.at[slot]
            )
            for k in range(count)
        ]

    n_up = experts // BLOCK
    per_chunk = groups // BLOCK

    def down_block(b):
        lb = b - n_up
        c = lb // per_chunk if lb < per_chunk * (n_chunks - 1) else n_chunks - 1
        return c, (lb - c * per_chunk) * BLOCK * per_slot

    def start_down(b):
        c, first = down_block(b)
        column, width = chunks[c]
        step = per_slot if width == WIDE else 2 * per_slot
        for i in range(BLOCK):
            for copy in load_down(first + i * step, column, width, (b * BLOCK + i) % RING):
                copy.start()

    barrier = pltpu.get_barrier_semaphore()
    for dev in device[1:]:
        pl.semaphore_signal(barrier, inc=1, device_id=dev, device_id_type=MESH)
    mine = [
        pltpu.make_async_copy(ids_hbm, ids_ref, own_sem.at[0]),
        pltpu.make_async_copy(gates_hbm, gates_ref, own_sem.at[1]),
        pltpu.make_async_copy(tok_hbm, xg.at[0], own_sem.at[2]),
    ]
    for copy in mine:
        copy.start()

    def message(i, src, dst, dev, group):
        return pltpu.make_async_remote_copy(
            src_ref=src, dst_ref=dst, send_sem=ssem.at[group], recv_sem=rsem.at[i], device_id=dev, device_id_type=MESH
        )

    low, high = pl.ds(0, half), pl.ds(half, half)
    sent = {
        TO_PARTNER: message(TO_PARTNER, xg.at[0], xg.at[1], partner, ROWS_SENT),
        X_LOW: message(X_LOW, xg.at[0, low], xg.at[2, low], xn, ROWS_SENT),
        X_HIGH: message(X_HIGH, xg.at[0, high], xg.at[2, high], xn, ROWS_SENT),
        Y_HIGH: message(Y_HIGH, xg.at[0, high], xg.at[4, high], yn, ROWS_SENT),
        Y_LOW: message(Y_LOW, xg.at[0, low], xg.at[4, low], yn, ROWS_SENT),
        DIAG_Y: message(DIAG_Y, xg.at[2, low], xg.at[6, low], yn, ROWS_SENT),
        DIAG_X: message(DIAG_X, xg.at[4, high], xg.at[6, high], xn, ROWS_SENT),
        PASS_X: message(PASS_X, xg.at[2], xg.at[3], partner, ROWS_SENT),
        PASS_Y: message(PASS_Y, xg.at[4], xg.at[5], partner, ROWS_SENT),
        PASS_D: message(PASS_D, xg.at[6], xg.at[7], partner, ROWS_SENT),
    }

    for r in range(1, SOURCES):
        hop = r == 1 or r % 2 == 0
        sent[META[r]] = message(META[r], mg.at[0 if hop else r - 1], mg.at[r], device[r] if hop else partner, META_SENT)

    for copy in mine:
        copy.wait()
    mg[0, 0:top_k, :] = ids_ref[...].astype(F32)
    mg[0, top_k:, :] = gates_ref[...]
    for s in range(RING):
        for copy in load_up(s, s):
            copy.start()
    pl.semaphore_wait(barrier, SOURCES - 1)
    for r in (6, 2, 4, 1):
        sent[META[r]].start()
    for i in (X_LOW, Y_HIGH, X_HIGH, Y_LOW, TO_PARTNER):
        sent[i].start()

    earlier = jnp.where(iota((tok, tok), 0) < iota((tok, tok), 1), 1.0, 0.0).astype(BF16)
    expert_row = (iota((experts, tok), 0) + first_expert).astype(F32)
    n_main = experts * MAIN
    n_rest = experts * 2 * rest
    row, col = iota((4 * experts, 4 * n_main), 0), iota((4 * experts, 4 * n_main), 1)
    spread[:, 0 : 4 * n_main] = jnp.where(row == col // MAIN, 1.0, 0.0).astype(BF16)
    row, col = iota((4 * experts, 4 * n_rest), 0), iota((4 * experts, 4 * n_rest), 1)
    spread[:, 4 * n_main :] = jnp.where(row == col // (2 * rest), 1.0, 0.0).astype(BF16)

    def route(r):
        hit = jnp.zeros((experts, tok), F32)
        gate = jnp.zeros((experts, tok), F32)
        for j in range(top_k):
            here = mg[r, j : j + 1, :] == expert_row
            hit = jnp.where(here, 1.0, hit)
            gate = jnp.where(here, mg[r, top_k + j : top_k + j + 1, :], gate)
        before = jnp.dot(hit.astype(BF16), earlier, preferred_element_type=F32)
        slot = jnp.where(hit > 0.5, before, NO_SLOT)
        val[r] = slot
        g_hi = gate.astype(BF16).astype(F32)
        g_mid = (gate - g_hi).astype(BF16).astype(F32)
        g_lo = gate - g_hi - g_mid
        stack = jnp.concatenate([slot, g_hi, g_mid, g_lo], axis=0)
        by_token = stack.T.astype(BF16)
        wide = jnp.dot(by_token, spread[...], preferred_element_type=F32)
        lane = iota((tok, n_main), 1)
        in_main = wide[:, 0:n_main] == (lane % MAIN).astype(F32)
        lane = iota((tok, n_rest), 1)
        want = jnp.where(lane // rest % 2 == r % 2, MAIN + lane % rest, -1)
        in_rest = wide[:, 4 * n_main : 4 * n_main + n_rest] == want.astype(F32)
        for k in range(1, 4):
            rows = pl.ds((k - 1) * tok, tok)
            piece = wide[:, k * n_main : (k + 1) * n_main]
            gmat[r, rows, 0:n_main] = jnp.where(in_main, piece, 0.0).astype(BF16)
            piece = wide[:, 4 * n_main + k * n_rest : 4 * n_main + (k + 1) * n_rest]
            gmat[r, rows, n_main:] = jnp.where(in_rest, piece, 0.0).astype(BF16)

    def one_hot(slots, want, e):
        line = jnp.broadcast_to(slots[e : e + 1, :], want.shape)
        return jnp.where(line == want, 1.0, 0.0).astype(BF16)

    def dispatch(sources, want, rows, batch, held=None):
        slots = jnp.concatenate([val[r] for r in sources], axis=1) if len(sources) > 1 else val[sources[0]]
        x = xg[sources[0] : sources[-1] + 1].reshape(len(sources) * tok, d_model)
        height = want.shape[0]
        for e in range(0, experts, batch):
            pick = jnp.concatenate([one_hot(slots, want, e + i) for i in range(batch)], axis=0)
            placed = jnp.dot(pick, x, preferred_element_type=F32)
            part = slice(e * height // tok, (e + batch) * height // tok)
            if held == "keep":
                away[part] = placed.reshape(-1, tok, d_model)
                continue
            if held == "add":
                placed += away[part].reshape(placed.shape)
            xe[e : e + batch, rows : rows + height, :] = placed.astype(BF16).reshape(batch, height, d_model)

    def dispatch_main(*sources):
        shape = (len(sources) * MAIN, len(sources) * tok)
        i, l = iota(shape, 0), iota(shape, 1)
        want = jnp.where(i // MAIN == l // tok, i % MAIN, -1).astype(F32)
        dispatch(sources, want, MAIN * sources[0], 16 // len(sources))

    def dispatch_rest(sources, held=None):
        q = sources[0] // 4
        shape = (4 * rest, len(sources) * tok)
        i, l = iota(shape, 0), iota(shape, 1)
        want = jnp.where(4 * q + i // rest == sources[0] + l // tok, MAIN + i % rest, -1).astype(F32)
        dispatch(sources, want, MAIN * SOURCES + 4 * rest * q, 16, held)

    def route_range(lo, hi):
        @pl.loop(lo, hi)
        def _(r):
            route(r)

    route_range(0, 1)
    sent[META[1]].wait_recv()
    route_range(1, 2)
    sent[TO_PARTNER].wait_recv()
    dispatch_main(0, 1)
    for r in range(2, SOURCES, 2):
        sent[META[r]].wait_recv()
        sent[META[r + 1]].start()
    for r in range(3, SOURCES, 2):
        sent[META[r]].wait_recv()
    route_range(2, 5)
    sent[X_LOW].wait_recv()
    sent[DIAG_Y].start()
    sent[Y_HIGH].wait_recv()
    sent[DIAG_X].start()
    route_range(5, 8)
    sent[X_HIGH].wait_recv()
    sent[PASS_X].start()
    sent[Y_LOW].wait_recv()
    sent[PASS_Y].start()
    dispatch_main(2)
    dispatch_main(4)
    sent[PASS_X].wait_recv()
    dispatch_main(3)
    sent[PASS_Y].wait_recv()
    dispatch_main(5)
    dispatch_rest((0, 1, 2, 3))
    sent[DIAG_Y].wait_recv()
    sent[DIAG_X].wait_recv()
    sent[PASS_D].start()
    dispatch_rest((4, 5), "keep")
    dispatch_main(6)
    sent[PASS_D].wait_recv()
    dispatch_main(7)
    dispatch_rest((6, 7), "add")

    full = ff // WIDE * WIDE

    def up_block(b):
        base = (b * BLOCK) % RING
        for i in range(BLOCK):
            wait_up(base + i)
        for i in range(BLOCK):
            e, slot = b * BLOCK + i, base + i
            x = xe[e]
            a = jnp.dot(x, ring[slot, 0, :, 0:full], preferred_element_type=F32)
            u = jnp.dot(x, ring[slot, 1, :, 0:full], preferred_element_type=F32)
            xe[e, :, 0:full] = (jax.nn.silu(a) * u).astype(BF16)
            tail = jnp.concatenate([ring[slot, 0, :, full:], ring[slot, 1, :, full:]], axis=1)
            t = jnp.dot(x, tail, preferred_element_type=F32)
            xe[e, :, full:ff] = (jax.nn.silu(t[:, : ff - full]) * t[:, ff - full :]).astype(BF16)

    ahead = RING // BLOCK

    for b in range(n_up):
        up_block(b)
        if b + ahead < n_up:
            for i in range(BLOCK):
                for copy in load_up((b + ahead) * BLOCK + i, (b * BLOCK) % RING + i):
                    copy.start()
        else:
            start_down(b + ahead)

    def wait_block(b, lo=0, hi=BLOCK):
        for i in range(lo, hi):
            wait_down((b * BLOCK + i) % RING)

    n_blocks = n_up + per_chunk * (n_chunks - 1) + 1

    def down(b, lo, hi):
        c, first = down_block(b)
        column, width = chunks[c]
        step = per_slot if width == WIDE else 2 * per_slot
        for i in range(lo, hi):
            for k in range(step):
                e = first + i * step + k
                w = down_view((b * BLOCK + i) % RING, k, width)[...]
                y = jnp.dot(xe[e, :, 0:ff], w, preferred_element_type=F32)
                xe[e, 0 : MAIN * SOURCES, ff : ff + width] = y[0 : MAIN * SOURCES].astype(BF16)
                yrest[e, :, 0:width] = y[MAIN * SOURCES :]
        if hi == BLOCK and b + ahead < n_blocks:
            start_down(b + ahead)

    def gated(r, c):
        width = chunks[c][1]
        top, bottom = MAIN * r, 2 * rest * (r // 2)
        y = jnp.concatenate(
            [
                xe[:, top : top + MAIN, ff : ff + width].reshape(n_main, width),
                yrest[:, bottom : bottom + 2 * rest, 0:width].reshape(n_rest, width).astype(BF16),
            ],
            axis=0,
        )
        s = jnp.dot(gmat[r], y, preferred_element_type=F32)
        return s[0:tok] + s[tok : 2 * tok] + s[2 * tok :]

    def cols(c):
        return pl.ds(*chunks[c])

    last = n_chunks - 1

    def sums(kind, c):
        i = FIRST_SUM + 5 * c + kind
        group = SUM_SENT + kind
        if kind == 0:
            return message(i, away.at[:, :, cols(c)], got.at[:, :, cols(c)], partner, group)
        if c == last:
            place, dev = ((XN, xn), (YN, yn), (DIAG, diag))[kind - 1]
            return message(i, home.at[place, :, cols(c)], direct.at[kind - 1], dev, LAST_SENT)
        if kind == 1:
            return message(i, home.at[pl.ds(XN, 2), low, cols(c)], rx1.at[:, :, cols(c)], xn, group)
        if kind == 2:
            return message(i, home.at[pl.ds(DIAG, 2), high, cols(c)], ry1.at[:, :, cols(c)], yn, group)
        if kind == 3:
            return message(i, via_y.at[:, cols(c)], ry2.at[:, cols(c)], yn, group)
        return message(i, via_x.at[:, cols(c)], rx2.at[:, cols(c)], xn, group)

    def combine_away(c):
        for r in range(1, SOURCES, 2):
            away[PLACE[r // 2], :, cols(c)] = gated(r, c)

    def combine_home(c):
        sums(0, c).start()
        for r in range(0, SOURCES, 2):
            home[PLACE[r // 2], :, cols(c)] = gated(r, c)

    def chip_sum(c):
        sums(0, c).wait_recv()
        for d in range(4):
            home[d, :, cols(c)] += got[d, :, cols(c)]
        for kind in (3, 1, 2) if c == last else (1, 2):
            sums(kind, c).start()

    def pass_on(c):
        sums(1, c).wait_recv()
        via_y[:, cols(c)] = home[YN, low, cols(c)] + rx1[1, :, cols(c)]
        sums(3, c).start()
        sums(2, c).wait_recv()
        via_x[:, cols(c)] = home[XN, high, cols(c)] + ry1[0, :, cols(c)]
        sums(4, c).start()

    def write(c):
        return pltpu.make_async_copy(result.at[:, cols(c)], out_hbm.at[:, cols(c)], out_sem)

    def finish(c):
        if c == last:
            total = home[OWN, :, cols(c)]
            for kind in (1, 2, 3):
                sums(kind, c).wait_recv()
                total += direct[kind - 1]
            result[:, cols(c)] = total.astype(BF16)
        else:
            sums(3, c).wait_recv()
            result[low, cols(c)] = (home[OWN, low, cols(c)] + rx1[0, :, cols(c)] + ry2[:, cols(c)]).astype(BF16)
            sums(4, c).wait_recv()
            result[high, cols(c)] = (home[OWN, high, cols(c)] + ry1[1, :, cols(c)] + rx2[:, cols(c)]).astype(BF16)
        write(c).start()

    def blocks(c):
        return range(n_up + c * per_chunk, min(n_up + (c + 1) * per_chunk, n_blocks))

    for c in range(n_chunks):
        first, *others = blocks(c)
        if c == 0:
            wait_block(first)
            down(first, 0, BLOCK)
        else:
            cut = BLOCK // 2 if c < last else BLOCK // 4
            wait_block(first, 0, cut)
            down(first, 0, cut)
            chip_sum(c - 1)
            wait_block(first, cut, BLOCK)
            for b in others:
                wait_block(b)
            down(first, cut, BLOCK)
        for b in others:
            if c == 0:
                wait_block(b)
            down(b, 0, BLOCK)
        if c >= 2:
            pass_on(c - 2)
        combine_away(c)
        combine_home(c)
    finish(0)
    chip_sum(last)
    pass_on(last - 1)
    for c in range(1, last - 1):
        finish(c)
    finish(last)
    finish(last - 1)

    most = pl.ds(0, chunks[last][0])
    for group, ref in (
        (META_SENT, mg.at[pl.ds(0, SOURCES - 1)]),
        (ROWS_SENT, xg.at[pl.ds(0, SOURCES - 1)]),
        (SUM_SENT, away),
        (SUM_SENT + 1, home.at[pl.ds(XN, 2), low, most]),
        (SUM_SENT + 2, home.at[pl.ds(DIAG, 2), high, most]),
        (SUM_SENT + 3, via_y.at[:, most]),
        (SUM_SENT + 4, via_x.at[:, most]),
        (LAST_SENT, home.at[pl.ds(XN, 3), :, cols(last)]),
    ):
        message(0, ref, ref, partner, group).wait_send()
    pltpu.make_async_copy(result, out_hbm, out_sem).wait()


def solution(mesh):
    ep_size, tp_size = mesh.shape["ep"], mesh.shape["tp"]
    row_spec = P(("dp", "ep", "tp"), None)

    def local_layer(tokens, expert_ids, gates, w_gate, w_up, w_down):
        tok, d_model = tokens.shape
        top_k = expert_ids.shape[1]
        experts, _, ff = w_gate.shape
        capacity = 5 * top_k * tok // (4 * experts * ep_size)
        assert (ep_size, tp_size, capacity, tok, experts) == (2, 4, MAIN + 4, 128, 32)
        n_main, n_rest = experts * MAIN, experts * 8
        rows = SOURCES * capacity
        n_chunks = -(-d_model // WIDE)
        n_msg = FIRST_SUM + 5 * n_chunks
        hbm = pl.BlockSpec(memory_space=pl.ANY)
        return pl.pallas_call(
            kernel,
            out_shape=jax.ShapeDtypeStruct((tok, d_model), BF16),
            in_specs=[hbm] * 6,
            out_specs=hbm,
            scratch_shapes=[
                pltpu.VMEM((top_k, tok), jnp.int32),
                pltpu.VMEM((top_k, tok), F32),
                pltpu.VMEM((SOURCES, tok, d_model), BF16),
                pltpu.VMEM((SOURCES, 2 * top_k, tok), F32),
                pltpu.VMEM((SOURCES, experts, tok), F32),
                pltpu.VMEM((4 * experts, 4 * (n_main + n_rest)), BF16),
                pltpu.VMEM((SOURCES, 3 * tok, n_main + n_rest), BF16),
                pltpu.VMEM((experts, rows, d_model), BF16),
                pltpu.VMEM((experts, rows - MAIN * SOURCES, WIDE), F32),
                pltpu.VMEM((RING, 2, d_model, ff), BF16),
                pltpu.VMEM((4, tok, d_model), F32),
                pltpu.VMEM((4, tok, d_model), F32),
                pltpu.VMEM((4, tok, d_model), F32),
                pltpu.VMEM((2, tok // 2, d_model), F32),
                pltpu.VMEM((2, tok // 2, d_model), F32),
                pltpu.VMEM((tok // 2, d_model), F32),
                pltpu.VMEM((tok // 2, d_model), F32),
                pltpu.VMEM((tok // 2, d_model), F32),
                pltpu.VMEM((tok // 2, d_model), F32),
                pltpu.VMEM((3, tok, d_model - WIDE * (n_chunks - 1)), F32),
                pltpu.VMEM((tok, d_model), BF16),
                pltpu.SemaphoreType.DMA((3,)),
                pltpu.SemaphoreType.DMA,
                pltpu.SemaphoreType.DMA((RING,)),
                pltpu.SemaphoreType.DMA((LAST_SENT + 1,)),
                pltpu.SemaphoreType.DMA((n_msg,)),
            ],
            compiler_params=pltpu.CompilerParams(
                collective_id=0, has_side_effects=True, vmem_limit_bytes=67043328
            ),
        )(expert_ids.T, gates.T, tokens, w_gate, w_up, w_down)

    return jax.shard_map(
        local_layer,
        mesh=mesh,
        in_specs=(row_spec, row_spec, row_spec, P("ep", None, "tp"), P("ep", None, "tp"), P("ep", "tp", None)),
        out_specs=row_spec,
        check_vma=False,
    )
```
